32 devices in a mesh: row: 4 (over z), col: 8 (over y, x, core).
Axes of the slice: x: 2, y: 2, z: 4, core: 2. Of those that a mesh axis runs over, the one named last changes fastest.
Arguments:
- features: bfloat16 [32768, 256], P(('row', 'col')), may hold values from -6 to 6
- tile_values: bfloat16 [4, 8, 256, 128, 128], P('row', 'col'), may hold values from -0.09375 to 0.09375
- tile_rows: int32 [4, 8, 256], P('row', 'col'), may hold values from 0 to 63, as said below
- tile_cols: int32 [4, 8, 256], P('row', 'col'), may hold values from 0 to 31, as said below
- tile_count: int32 [4, 8], P('row', 'col'), may hold values from 64 to 256, as said below
- w_first: bfloat16 [256, 256], replicated, may hold values from -0.375 to 0.375
- w_second: bfloat16 [256, 256], replicated, may hold values from -0.375 to 0.375
Outputs:
- output: bfloat16 [32768, 256], P(('row', 'col'))
The draws below stay inside these ranges and needn't reach their ends.
Inputs may be any that keep to these rules, and one draw needn't show every extreme that they name: `tile_rows`: in each block the slots name distinct tiles; the first tile_count slots are ordered by tile column, then tile row; later slots are padding. `tile_cols`: as for tile_rows. `tile_count`: some block uses all 256 slots.
All inputs are finite; a program needn't handle non-finite values.
Results may differ from the reference program's by a relative error of at most 0.024.
Values may be sent and summed in bfloat16 or wider, within the bound.
A program may use at most 192 MiB of HBM per device.

```python
import jax
import jax.numpy as jnp
from jax import lax

F = 256
TILE = 128
NODE_DEV = 1024
TILES = 256
TILE_ROWS = 64
TILE_COLS = 32
NODES = 32768
N_ROW = 4
N_COL = 8


def tile_layout(key):
    device_total = N_ROW * N_COL
    slots_total = TILE_ROWS * TILE_COLS
    layout_key = jax.random.fold_in(key, 4242)
    heaviest = jax.random.randint(jax.random.fold_in(layout_key, 1), (), 0, device_total)
    others = jax.random.randint(jax.random.fold_in(layout_key, 2), (device_total,), TILES // 4, TILES + 1)
    counts = jnp.where(jnp.arange(device_total, dtype=jnp.int32) == heaviest, TILES, others).astype(jnp.int32)

    def one_block(device, filled):
        chosen = jax.random.permutation(jax.random.fold_in(layout_key, 100 + device), slots_total)[:TILES]
        slot_ids = jnp.arange(TILES, dtype=jnp.int32)
        marked = jnp.where(slot_ids < filled, chosen, chosen + slots_total).astype(jnp.int32)
        ordered = jnp.sort(marked)
        flat_index = ordered % slots_total
        return (flat_index % TILE_ROWS, flat_index // TILE_ROWS)
    row_ids, col_ids = jax.vmap(one_block)(jnp.arange(device_total, dtype=jnp.int32), counts)
    return (row_ids.reshape(N_ROW, N_COL, TILES).astype(jnp.int32), col_ids.reshape(N_ROW, N_COL, TILES).astype(jnp.int32), counts.reshape(N_ROW, N_COL))


def draw_tile_rows(key, part):
    return tile_layout(key)[0]


def draw_tile_cols(key, part):
    return tile_layout(key)[1]


def draw_tile_count(key, part):
    return tile_layout(key)[2]


def block_levels(rng, shape, pieces, least, largest):
    def one(axis_at, parts):
        draws = jax.random.uniform(jax.random.fold_in(jax.random.fold_in(rng, 6), axis_at), (parts,), jnp.float32, least / len(pieces), largest / len(pieces))
        return jnp.repeat(jnp.exp(draws), shape[axis_at] // parts).reshape((-1,) + (1,) * (len(shape) - axis_at - 1))

    factor_of = one(*pieces[0])
    for cut in pieces[1:]:
        factor_of = factor_of * one(*cut)
    return factor_of


def centred(own_key, extent, width, most, cuts=(), held_as=jnp.bfloat16):
    drawn = jax.random.normal(own_key, extent, jnp.float32) * width
    if len(cuts) > 0:
        drawn = block_levels(own_key, extent, cuts, -0.22, 0.18) * drawn
    return jnp.clip(drawn, min=-most, max=most).astype(held_as)


def setup_inputs(seed: int = 0) -> dict:
    key_of = jax.random.split(jax.random.key(seed), 8)
    return {
        "features": centred(key_of[0], (NODES, F), 1.0, 6.0, ((0, 32),)),
        "tile_values": centred(key_of[1], (N_ROW, N_COL, TILES, TILE, TILE), (TILES * TILE * TILE // NODE_DEV) ** -0.5, 0.09375, ((0, 4), (1, 8))),
        "tile_rows": draw_tile_rows(jax.random.fold_in(key_of[7], 71), 0),
        "tile_cols": draw_tile_cols(jax.random.fold_in(key_of[7], 71), 0),
        "tile_count": draw_tile_count(jax.random.fold_in(key_of[7], 71), 0),
        "w_first": centred(key_of[5], (F, F), F ** -0.5, 0.375),
        "w_second": centred(key_of[6], (F, F), F ** -0.5, 0.375),
    }


def block_partial(values, row_ids, col_ids, filled, panel_tiles):
    active = (jnp.arange(TILES, dtype=jnp.int32) < filled).astype(jnp.float32)
    inputs = panel_tiles[col_ids].astype(jnp.float32)
    products = jnp.einsum("gij,gjf->gif", values.astype(jnp.float32), inputs) * active[:, None, None]
    return jax.ops.segment_sum(products, row_ids, num_segments=TILE_ROWS)


def aggregate(inputs_now, tile_values, tile_rows, tile_cols, tile_count):
    blocks = inputs_now.reshape(N_ROW, N_COL, NODE_DEV, F)

    def row_block(row_index):
        def add_col(running, col_index):
            panel_tiles = blocks[:, col_index].reshape(N_ROW * NODE_DEV // TILE, TILE, F)
            partial_value = block_partial(tile_values[row_index, col_index], tile_rows[row_index, col_index],
                                    tile_cols[row_index, col_index], tile_count[row_index, col_index], panel_tiles)
            rounded = lax.optimization_barrier(partial_value.astype(jnp.bfloat16))
            return running + rounded.astype(jnp.float32), None

        running, unused = lax.scan(add_col, jnp.zeros((TILE_ROWS, TILE, F), jnp.float32),
                                   jnp.arange(N_COL, dtype=jnp.int32))
        return running.astype(jnp.bfloat16)

    summed = lax.map(row_block, jnp.arange(N_ROW, dtype=jnp.int32))
    return summed.reshape(N_ROW * N_COL * NODE_DEV, F)


def reference(features, tile_values, tile_rows, tile_cols, tile_count, w_first, w_second):
    summed = aggregate(features, tile_values, tile_rows, tile_cols, tile_count)
    hidden = jax.nn.relu(jnp.dot(summed, w_first, preferred_element_type=jnp.float32)).astype(jnp.bfloat16)
    summed_two = aggregate(hidden, tile_values, tile_rows, tile_cols, tile_count)
    return jax.nn.relu(jnp.dot(summed_two, w_second, preferred_element_type=jnp.float32)).astype(jnp.bfloat16)
```

```python
import functools

import jax
import jax.numpy as jnp
from jax import lax
from jax.experimental import pallas as pl
from jax.experimental.pallas import tpu as pltpu
from jax.sharding import PartitionSpec as P

LANES = 128
UNROLL = 8
LOADS = 4
ROWS_AT_ONCE = 256
MESH = pl.DeviceIdType.MESH


def pair_plan(row_ids, col_ids, filled, row_tiles):
    slots = row_ids.shape[0]
    pairs_total = (slots + row_tiles) // 2
    slot_ids = jnp.arange(slots, dtype=jnp.int32)
    tile_ids = jnp.arange(row_tiles, dtype=jnp.int32)
    active = slot_ids < filled
    rows = jnp.where(active, row_ids, -1)
    earlier = (rows[:, None] == rows[None, :]) & (slot_ids[None, :] < slot_ids[:, None])
    rank = jnp.sum(earlier.astype(jnp.int32), axis=1)
    hit = (rows[:, None] == tile_ids[None, :]).astype(jnp.int32)
    count = jnp.sum(hit, axis=0)
    pairs = (count + 1) // 2
    start = jnp.sum(jnp.where(tile_ids[None, :] < tile_ids[:, None], pairs[None, :], 0), axis=1)
    place = jnp.where(active, 2 * jnp.sum(hit * start[None, :], axis=1) + rank, -1)
    places = jnp.arange(2 * pairs_total, dtype=jnp.int32)
    here = (places[:, None] == place[None, :]).astype(jnp.int32)
    slot_at = slots + jnp.sum(here * (slot_ids - slots)[None, :], axis=1)
    col_at = jnp.sum(here * col_ids[None, :], axis=1)
    pair_ids = jnp.arange(pairs_total, dtype=jnp.int32)
    opens = jnp.any((pair_ids[:, None] == start[None, :]) & (count > 0)[None, :], axis=1)
    keep = jnp.where(opens, 0.0, 1.0).astype(jnp.float32)
    last = jnp.where(count > 0, start + pairs - 1, pairs_total)
    return slot_at, col_at, keep, last


def kernel(n_row, n_col, chunks, slot_at, col_at, keep, last, feat, w1, w2, vals_hbm, out, *scratch):
    phases = 2 * chunks
    panels = scratch[:phases]
    core_in = scratch[phases : 2 * phases]
    step_in = scratch[2 * phases : 3 * phases]
    vals, sums, part, agg, load_sem, g_send, g_recv, c_send, c_recv, s_send, s_recv = scratch[
        3 * phases :
    ]
    slots, tile, _ = vals_hbm.shape
    node_dev, width = feat.shape
    pairs_total = keep.shape[0]
    per_dev = node_dev // tile
    half_tiles = per_dev // 2
    n_q = n_col // 2
    steps = n_q.bit_length() - 1
    block = half_tiles * tile
    half_rows = n_q * block
    r, c = lax.axis_index("row"), lax.axis_index("col")
    b0 = lax.rem(c, 2)
    q = lax.div(c, 2)

    barrier = pltpu.get_barrier_semaphore()
    partners = []
    for bit in range(steps + 1):
        mine = lax.rem(lax.div(c, 1 << bit), 2)
        partners.append((r, c + (1 - 2 * mine) * (1 << bit)))
    for device in partners:
        pl.semaphore_signal(barrier, inc=1, device_id=device, device_id_type=MESH)

    @pl.when(r > 0)
    def _():
        pl.semaphore_signal(barrier, inc=1, device_id=(r - 1, c), device_id_type=MESH)

    @pl.when(r < n_row - 1)
    def _():
        pl.semaphore_signal(barrier, inc=1, device_id=(r + 1, c), device_id_type=MESH)

    share = slots // LOADS
    loads = [
        pltpu.make_async_copy(
            vals_hbm.at[pl.ds(i * share, share)], vals.at[pl.ds(i * share, share)], load_sem.at[i]
        )
        for i in range(LOADS)
    ]
    for load in loads:
        load.start()

    def own(phase, offset, rows):
        return panels[phase].at[pl.ds(r * per_dev + offset, rows)]

    def project(chunk):
        def body(i, carry):
            at = pl.multiple_of(i * ROWS_AT_ONCE, ROWS_AT_ONCE)
            product = jnp.dot(
                feat[pl.ds(at, ROWS_AT_ONCE), :],
                w1[:, chunk * LANES : (chunk + 1) * LANES],
                preferred_element_type=jnp.float32,
            )
            tiles = ROWS_AT_ONCE // tile
            own(chunk, i * tiles, tiles)[...] = product.astype(jnp.bfloat16).reshape(
                tiles, tile, LANES
            )
            return carry

        lax.fori_loop(0, node_dev // ROWS_AT_ONCE, body, 0)

    project(0)
    neighbours = (r > 0).astype(jnp.int32) + (r < n_row - 1).astype(jnp.int32)
    pl.semaphore_wait(barrier, len(partners) + neighbours)

    def hop_copy(phase, way, hop, node, device):
        view = panels[phase].at[pl.ds(node * per_dev, per_dev)]
        return pltpu.make_async_remote_copy(
            src_ref=view,
            dst_ref=view,
            send_sem=g_send.at[phase, way, hop - 1],
            recv_sem=g_recv.at[phase, way, hop - 1],
            device_id=(device, c),
            device_id_type=MESH,
        )

    def sends(phase, hop):
        yield (r < n_row - 1) & (r >= hop - 1), lambda: hop_copy(phase, 0, hop, r - hop + 1, r + 1)
        yield (r > 0) & (r + hop <= n_row), lambda: hop_copy(phase, 1, hop, r + hop - 1, r - 1)

    def hop_start(phase, hop):
        for cond, make in sends(phase, hop):

            @pl.when(cond)
            def _(make=make):
                make().start()

    def hop_wait(phase, hop):
        @pl.when(r >= hop)
        def _():
            hop_copy(phase, 0, hop, r - hop, r).wait_recv()

        @pl.when(r + hop < n_row)
        def _():
            hop_copy(phase, 1, hop, r + hop, r).wait_recv()

    def hop_drain(phase, hop):
        for cond, make in sends(phase, hop):

            @pl.when(cond)
            def _(make=make):
                make().wait_send()

    class Gather:
        def __init__(self, phase):
            self.phase, self.hop = phase, 0

        def advance(self):
            if self.phase >= phases or self.hop >= n_row - 1:
                return
            if self.hop > 0:
                hop_wait(self.phase, self.hop)
            self.hop += 1
            hop_start(self.phase, self.hop)

        def finish(self):
            if self.phase >= phases:
                return
            while self.hop < n_row - 1:
                self.advance()
            hop_wait(self.phase, n_row - 1)
            for hop in range(1, n_row):
                hop_drain(self.phase, hop)

    def compute(phase, low, high, total):
        panel = panels[phase]

        def one(p, acc):
            left = [vals[slot_at[2 * p + k]] for k in range(2)]
            right = [panel[col_at[2 * p + k]] for k in range(2)]
            product = jnp.dot(
                jnp.concatenate(left, axis=1),
                jnp.concatenate(right, axis=0),
                preferred_element_type=jnp.float32,
            )
            acc = acc * keep[p] + product
            sums[p] = acc.astype(jnp.bfloat16)
            return acc

        def body(i, acc):
            for u in range(UNROLL):
                acc = one(i * UNROLL + u, acc)
            return acc

        return lax.fori_loop(low // UNROLL, high // UNROLL, body, total)

    def place_rows():
        def body(i, carry):
            dest, h = lax.div(i, 2), lax.rem(i, 2)
            dq = lax.div(dest, 2)
            rev = sum(lax.rem(lax.div(dq, 1 << k), 2) * (1 << (steps - 1 - k)) for k in range(steps))
            at = rev * (1 - h) + dq * h
            base = ((lax.rem(dest, 2) * 2 + h) * n_q + at) * half_tiles
            for t in range(half_tiles):
                row_tile = dest * per_dev + h * half_tiles + t
                part[pl.ds(pl.multiple_of((base + t) * tile, tile), tile), :] = sums[last[row_tile]]
            return carry

        lax.fori_loop(0, 2 * n_col, body, 0)

    def add_in(at, source, source_at, rows):
        piece = min(rows, ROWS_AT_ONCE)

        def body(i, carry):
            here = pl.ds(pl.multiple_of(at + i * piece, tile), piece)
            there = pl.ds(pl.multiple_of(source_at + i * piece, tile), piece)
            added = part[here, :].astype(jnp.float32) + source[there, :].astype(jnp.float32)
            part[here, :] = added.astype(jnp.bfloat16)
            return carry

        lax.fori_loop(0, rows // piece, body, 0)

    def remote(src, dst, send_sem, recv_sem, device):
        return pltpu.make_async_remote_copy(
            src_ref=src,
            dst_ref=dst,
            send_sem=send_sem,
            recv_sem=recv_sem,
            device_id=device,
            device_id_type=MESH,
        )

    def rows_at(ref, at, rows):
        return ref.at[pl.ds(pl.multiple_of(at, tile), rows)]

    def reduce(phase, gather):
        first = [
            remote(
                rows_at(part, ((1 - b0) * 2 + h) * half_rows, half_rows),
                core_in[phase].at[pl.ds(h * half_rows, half_rows)],
                c_send.at[phase, h],
                c_recv.at[phase, h],
                partners[0],
            )
            for h in range(2)
        ]
        started = list(first)
        for copy in first:
            copy.start()
        gather.advance()
        base = [(b0 * 2 + h) * half_rows for h in range(2)]
        size = half_rows
        arrived = [(first[h], core_in[phase], h * half_rows) for h in range(2)]
        for step in range(steps):
            following = []
            for h in range(2):
                copy, source, source_at = arrived[h]
                copy.wait_recv()
                add_in(base[h], source, source_at, size)
                bit = step if h == 0 else steps - 1 - step
                mine = lax.rem(lax.div(q, 1 << bit), 2)
                landing = (h * (n_q - 1) + n_q - (n_q >> step)) * block
                copy = remote(
                    rows_at(part, base[h] + (1 - mine) * (size // 2), size // 2),
                    step_in[phase].at[pl.ds(landing, size // 2)],
                    s_send.at[phase, h, step],
                    s_recv.at[phase, h, step],
                    partners[1 + bit],
                )
                copy.start()
                started.append(copy)
                base[h] = base[h] + mine * (size // 2)
                following.append((copy, step_in[phase], landing))
            size //= 2
            arrived = following
            gather.advance()
        for h in range(2):
            copy, source, source_at = arrived[h]
            copy.wait_recv()
            here = pl.ds(pl.multiple_of(base[h], tile), block)
            added = part[here, :].astype(jnp.float32) + source[
                pl.ds(source_at, block), :
            ].astype(jnp.float32)
            if phase < chunks:
                hidden = jnp.maximum(added, 0.0).astype(jnp.bfloat16)
                own(phase + chunks, h * half_tiles, half_tiles)[...] = hidden.reshape(
                    half_tiles, tile, LANES
                )
            else:
                agg[phase - chunks, pl.ds(h * block, block), :] = added.astype(jnp.bfloat16)
        for copy in started:
            copy.wait_send()

    vals[slots] = jnp.zeros((tile, tile), vals.dtype)
    sums[pairs_total] = jnp.zeros((tile, LANES), sums.dtype)
    gather = Gather(0)
    gather.advance()
    for chunk in range(1, chunks):
        project(chunk)
    for load in loads:
        load.wait()
    gather.finish()
    for phase in range(phases):
        gather = Gather(phase + 1)
        gather.advance()
        total = jnp.zeros((tile, LANES), jnp.float32)
        compute(phase, 0, pairs_total, total)
        place_rows()
        reduce(phase, gather)
        gather.finish()

    def finish(i, carry):
        here = pl.ds(pl.multiple_of(i * ROWS_AT_ONCE, ROWS_AT_ONCE), ROWS_AT_ONCE)
        whole = jnp.concatenate([agg[chunk, here, :] for chunk in range(chunks)], axis=1)
        product = jnp.dot(whole, w2[...], preferred_element_type=jnp.float32)
        out[here, :] = jnp.maximum(product, 0.0).astype(out.dtype)
        return carry

    lax.fori_loop(0, node_dev // ROWS_AT_ONCE, finish, 0)


def shards(n_row, n_col, features, tile_values, tile_rows, tile_cols, tile_count, w_first, w_second):
    slots, tile = tile_values.shape[2], tile_values.shape[-1]
    node_dev, width = features.shape
    row_tiles = node_dev * n_col // tile
    chunks = width // LANES
    phases = 2 * chunks
    pairs_total = (slots + row_tiles) // 2
    n_q = n_col // 2
    steps = n_q.bit_length() - 1
    plan = pair_plan(tile_rows[0, 0], tile_cols[0, 0], tile_count[0, 0], row_tiles)
    half = node_dev // 2
    vmem = pl.BlockSpec(memory_space=pltpu.VMEM)
    smem = pl.BlockSpec(memory_space=pltpu.SMEM)
    bf16 = jnp.bfloat16
    dma = pltpu.SemaphoreType.DMA
    return pl.pallas_call(
        functools.partial(kernel, n_row, n_col, chunks),
        name="gcn",
        out_shape=jax.ShapeDtypeStruct((node_dev, width), bf16),
        in_specs=[smem] * 4 + [vmem] * 3 + [pl.BlockSpec(memory_space=pltpu.HBM)],
        out_specs=vmem,
        scratch_shapes=[pltpu.VMEM((n_row * node_dev // tile, tile, LANES), bf16)] * phases
        + [pltpu.VMEM((2 * n_q * half, LANES), bf16)] * phases
        + [pltpu.VMEM((2 * (n_q - 1) * half, LANES), bf16)] * phases
        + [
            pltpu.VMEM((slots + 1, tile, tile), bf16),
            pltpu.VMEM((pairs_total + 1, tile, LANES), bf16),
            pltpu.VMEM((n_col * node_dev, LANES), bf16),
            pltpu.VMEM((chunks, node_dev, LANES), bf16),
            dma((LOADS,)),
            dma((phases, 2, n_row - 1)),
            dma((phases, 2, n_row - 1)),
            dma((phases, 2)),
            dma((phases, 2)),
            dma((phases, 2, steps)),
            dma((phases, 2, steps)),
        ],
        compiler_params=pltpu.CompilerParams(
            collective_id=0, has_side_effects=True, vmem_limit_bytes=63 * 1024 * 1024
        ),
    )(*plan, features, w_first, w_second, tile_values[0, 0])


def solution(mesh):
    return jax.shard_map(
        functools.partial(shards, mesh.shape["row"], mesh.shape["col"]),
        mesh=mesh,
        in_specs=(
            P(("row", "col"), None),
            P("row", "col", None, None, None),
            P("row", "col", None),
            P("row", "col", None),
            P("row", "col"),
            P(),
            P(),
        ),
        out_specs=P(("row", "col"), None),
        check_vma=False,
    )
```

```python
import functools

import jax
import jax.numpy as jnp
from jax import lax
from jax.experimental import pallas as pl
from jax.experimental.pallas import tpu as pltpu
from jax.sharding import PartitionSpec as P

LANES = 128
UNROLL = 8
LOADS = 4
ROWS_AT_ONCE = 256
MESH = pl.DeviceIdType.MESH


def iota(shape, axis):
    return lax.broadcasted_iota(jnp.int32, shape, axis)


def pair_plan(row_ids, col_ids, filled, row_tiles, pairs_total, width):
    slots = row_ids.shape[1]
    one, zero = jnp.int32(1), jnp.int32(0)

    def down(mask):
        return jnp.sum(mask, axis=0, keepdims=True)

    def across(mask):
        return jnp.sum(mask, axis=1, keepdims=True)

    square = (slots, slots)
    lane, sub = iota(square, 1), iota(square, 0)
    rows_l = jnp.where(iota((1, slots), 1) < filled, row_ids, -1)
    rows_s = across(jnp.where(lane == sub, rows_l, zero))
    cols_s = across(jnp.where(lane == sub, col_ids, zero))
    rank_s = across(jnp.where((rows_s == rows_l) & (lane < sub), one, zero))
    hit = jnp.where(rows_s == iota((slots, row_tiles), 1), one, zero)
    hit_t = jnp.where(rows_l == iota((row_tiles, slots), 0), one, zero)
    count_l, count_s = down(hit), across(hit_t)
    pairs_l, pairs_s = (count_l + 1) >> 1, (count_s + 1) >> 1
    box = (row_tiles, row_tiles)
    start_l = down(jnp.where(iota(box, 0) < iota(box, 1), pairs_s, zero))
    start_s = across(jnp.where(iota(box, 1) < iota(box, 0), pairs_l, zero))
    place_s = jnp.where(rows_s >= 0, 2 * across(hit * start_l) + rank_s, -one)
    here = place_s == iota((slots, width), 1)
    slot_ids = iota((slots, width), 0)
    slot_at = slots + down(jnp.where(here, slot_ids - slots, zero))
    col_at = down(jnp.where(here, cols_s, zero))
    opens = (start_s == iota((row_tiles, width), 1)) & (count_s > 0)
    keep = one - down(jnp.where(opens, one, zero))
    last = jnp.where(count_l > 0, start_l + pairs_l - 1, jnp.int32(pairs_total))
    return slot_at, col_at, keep.astype(jnp.float32), last


def kernel(n_row, n_col, chunks, pairs_total, filled, row_ids, col_ids, feat, w1, vals_hbm, out, *scratch):
    phases = 2 * chunks
    panels = scratch[:phases]
    core_in = scratch[phases : 2 * phases]
    step_in = scratch[2 * phases : 3 * phases]
    vals, sums, part, plan_v, keep_v, plan, keep, plan_sem = scratch[3 * phases : 3 * phases + 8]
    load_sem, g_send, g_recv, c_send, c_recv, s_send, s_recv = scratch[3 * phases + 8 :]
    slots, tile, _ = vals_hbm.shape
    node_dev, width = feat.shape
    per_dev = node_dev // tile
    half_tiles = per_dev // 2
    n_q = n_col // 2
    steps = n_q.bit_length() - 1
    block = half_tiles * tile
    half_rows = n_q * block
    r, c = lax.axis_index("row"), lax.axis_index("col")
    b0 = lax.rem(c, 2)
    q = lax.div(c, 2)

    barrier = pltpu.get_barrier_semaphore()
    partners = []
    for bit in range(steps + 1):
        mine = lax.rem(lax.div(c, 1 << bit), 2)
        partners.append((r, c + (1 - 2 * mine) * (1 << bit)))
    for device in partners:
        pl.semaphore_signal(barrier, inc=1, device_id=device, device_id_type=MESH)

    @pl.when(r > 0)
    def _():
        pl.semaphore_signal(barrier, inc=1, device_id=(r - 1, c), device_id_type=MESH)

    @pl.when(r < n_row - 1)
    def _():
        pl.semaphore_signal(barrier, inc=1, device_id=(r + 1, c), device_id_type=MESH)

    share = slots // LOADS
    loads = [
        pltpu.make_async_copy(
            vals_hbm.at[pl.ds(i * share, share)], vals.at[pl.ds(i * share, share)], load_sem.at[i]
        )
        for i in range(LOADS)
    ]
    for load in loads:
        load.start()

    def own(phase, offset, rows):
        return panels[phase].at[pl.ds(r * per_dev + offset, rows)]

    def project(chunk):
        def body(i, carry):
            at = pl.multiple_of(i * ROWS_AT_ONCE, ROWS_AT_ONCE)
            product = jnp.dot(
                feat[pl.ds(at, ROWS_AT_ONCE), :],
                w1[:, chunk * LANES : (chunk + 1) * LANES],
                preferred_element_type=jnp.float32,
            )
            tiles = ROWS_AT_ONCE // tile
            own(chunk, i * tiles, tiles)[...] = product.astype(jnp.bfloat16).reshape(
                tiles, tile, LANES
            )
            return carry

        lax.fori_loop(0, node_dev // ROWS_AT_ONCE, body, 0)

    project(0)
    neighbours = (r > 0).astype(jnp.int32) + (r < n_row - 1).astype(jnp.int32)
    pl.semaphore_wait(barrier, len(partners) + neighbours)

    def hop_copy(phase, way, hop, node, device):
        view = panels[phase].at[pl.ds(node * per_dev, per_dev)]
        return pltpu.make_async_remote_copy(
            src_ref=view,
            dst_ref=view,
            send_sem=g_send.at[phase, way, hop - 1],
            recv_sem=g_recv.at[phase, way, hop - 1],
            device_id=(device, c),
            device_id_type=MESH,
        )

    def sends(phase, hop):
        yield (r < n_row - 1) & (r >= hop - 1), lambda: hop_copy(phase, 0, hop, r - hop + 1, r + 1)
        yield (r > 0) & (r + hop <= n_row), lambda: hop_copy(phase, 1, hop, r + hop - 1, r - 1)

    def hop_start(phase, hop):
        for cond, make in sends(phase, hop):

            @pl.when(cond)
            def _(make=make):
                make().start()

    def hop_wait(phase, hop):
        @pl.when(r >= hop)
        def _():
            hop_copy(phase, 0, hop, r - hop, r).wait_recv()

        @pl.when(r + hop < n_row)
        def _():
            hop_copy(phase, 1, hop, r + hop, r).wait_recv()

    def hop_drain(phase, hop):
        for cond, make in sends(phase, hop):

            @pl.when(cond)
            def _(make=make):
                make().wait_send()

    class Gather:
        def __init__(self, phase):
            self.phase, self.hop = phase, 0

        def advance(self):
            if self.phase >= phases or self.hop >= n_row - 1:
                return
            if self.hop > 0:
                hop_wait(self.phase, self.hop)
            self.hop += 1
            hop_start(self.phase, self.hop)

        def finish(self):
            if self.phase >= phases:
                return
            while self.hop < n_row - 1:
                self.advance()
            hop_wait(self.phase, n_row - 1)
            for hop in range(1, n_row):
                hop_drain(self.phase, hop)

    def compute(phase, low, high, total):
        panel = panels[phase]

        def one(p, acc):
            left = [vals[plan[0, 2 * p + k]] for k in range(2)]
            right = [panel[plan[1, 2 * p + k]] for k in range(2)]
            product = jnp.dot(
                jnp.concatenate(left, axis=1),
                jnp.concatenate(right, axis=0),
                preferred_element_type=jnp.float32,
            )
            acc = acc * keep[0, p] + product
            sums[p] = acc.astype(jnp.bfloat16)
            return acc

        def body(i, acc):
            for u in range(UNROLL):
                acc = one(i * UNROLL + u, acc)
            return acc

        return lax.fori_loop(low // UNROLL, high // UNROLL, body, total)

    def place_rows(parity):
        def body(i, carry):
            dq, h = lax.div(i, 2), lax.rem(i, 2)
            dest = 2 * dq + parity
            rev = sum(lax.rem(lax.div(dq, 1 << k), 2) * (1 << (steps - 1 - k)) for k in range(steps))
            at = rev * (1 - h) + dq * h
            base = ((parity * 2 + h) * n_q + at) * half_tiles
            for t in range(half_tiles):
                row_tile = dest * per_dev + h * half_tiles + t
                part[pl.ds(pl.multiple_of((base + t) * tile, tile), tile), :] = sums[
                    plan[2, row_tile]
                ]
            return carry

        lax.fori_loop(0, 2 * n_q, body, 0)

    def add_in(at, source, source_at, rows):
        piece = min(rows, ROWS_AT_ONCE)

        def body(i, carry):
            here = pl.ds(pl.multiple_of(at + i * piece, tile), piece)
            there = pl.ds(pl.multiple_of(source_at + i * piece, tile), piece)
            added = part[here, :].astype(jnp.float32) + source[there, :].astype(jnp.float32)
            part[here, :] = added.astype(jnp.bfloat16)
            return carry

        lax.fori_loop(0, rows // piece, body, 0)

    def remote(src, dst, send_sem, recv_sem, device):
        return pltpu.make_async_remote_copy(
            src_ref=src,
            dst_ref=dst,
            send_sem=send_sem,
            recv_sem=recv_sem,
            device_id=device,
            device_id_type=MESH,
        )

    def rows_at(ref, at, rows):
        return ref.at[pl.ds(pl.multiple_of(at, tile), rows)]

    def mine_at(h, step):
        return lax.rem(lax.div(q, 1 << (step if h == 0 else steps - 1 - step)), 2)

    def pieces(h, step, size):
        if step >= steps:
            return [(0, size)]
        mine = mine_at(h, step)
        return [((1 - mine) * (size // 2), size // 2), (mine * (size // 2), size // 2)]

    def reduce(phase, gather):
        place_rows(1 - b0)
        started = []
        cuts = [pieces(h, 0, half_rows) for h in range(2)]
        arrived = [[], []]
        for k in range(len(cuts[0])):
            for h in range(2):
                off, rows = cuts[h][k]
                copy = remote(
                    rows_at(part, ((1 - b0) * 2 + h) * half_rows + off, rows),
                    rows_at(core_in[phase], h * half_rows + off, rows),
                    c_send.at[phase, h, k],
                    c_recv.at[phase, h, k],
                    partners[0],
                )
                copy.start()
                started.append(copy)
                arrived[h].append((copy, core_in[phase], h * half_rows + off, off, rows))
        place_rows(b0)
        gather.advance()
        base = [(b0 * 2 + h) * half_rows for h in range(2)]

        def take(h, k):
            copy, source, source_at, off, rows = arrived[h][k]
            copy.wait_recv()
            add_in(base[h] + off, source, source_at, rows)

        size = half_rows
        for step in range(steps):
            following = [[], []]
            for h in range(2):
                take(h, 0)
                bit = step if h == 0 else steps - 1 - step
                away = base[h] + (1 - mine_at(h, step)) * (size // 2)
                landing = (h * (n_q - 1) + n_q - (n_q >> step)) * block
                for k, (off, rows) in enumerate(pieces(h, step + 1, size // 2)):
                    copy = remote(
                        rows_at(part, away + off, rows),
                        rows_at(step_in[phase], landing + off, rows),
                        s_send.at[phase, h, step, k],
                        s_recv.at[phase, h, step, k],
                        partners[1 + bit],
                    )
                    copy.start()
                    started.append(copy)
                    following[h].append((copy, step_in[phase], landing + off, off, rows))
            for h in range(2):
                take(h, 1)
                base[h] = base[h] + mine_at(h, step) * (size // 2)
            size //= 2
            arrived = following
            gather.advance()
        for h in range(2):
            copy, source, source_at, off, rows = arrived[h][0]
            copy.wait_recv()
            here = pl.ds(pl.multiple_of(base[h], tile), block)
            there = pl.ds(pl.multiple_of(source_at, tile), block)
            added = part[here, :].astype(jnp.float32) + source[there, :].astype(jnp.float32)
            if phase < chunks:
                hidden = jnp.maximum(added, 0.0).astype(jnp.bfloat16)
                own(phase + chunks, h * half_tiles, half_tiles)[...] = hidden.reshape(
                    half_tiles, tile, LANES
                )
            else:
                at = (phase - chunks) * LANES
                out[h * block : (h + 1) * block, at : at + LANES] = added.astype(jnp.bfloat16)
        return started

    vals[slots] = jnp.zeros((tile, tile), vals.dtype)
    sums[pairs_total] = jnp.zeros((tile, LANES), sums.dtype)
    gather = Gather(0)
    gather.advance()
    for chunk in range(1, chunks):
        project(chunk)
    slot_at, col_at, keep_at, last = pair_plan(
        row_ids[...], col_ids[...], filled[0, 0], n_col * per_dev, pairs_total, plan.shape[1]
    )
    plan_v[0:1, :] = slot_at
    plan_v[1:2, :] = col_at
    plan_v[2:3, : last.shape[1]] = last
    keep_v[0:1, :] = keep_at
    moves = [
        pltpu.make_async_copy(plan_v, plan, plan_sem.at[0]),
        pltpu.make_async_copy(keep_v, keep, plan_sem.at[1]),
    ]
    gather.advance()
    for move in moves:
        move.start()
    for move in moves:
        move.wait()
    for load in loads:
        load.wait()
    following = Gather(1)
    while gather.hop < n_row - 1:
        gather.advance()
    following.advance()
    gather.finish()
    for phase in range(phases):
        gather, following = following, Gather(phase + 2)
        compute(phase, 0, pairs_total, jnp.zeros((tile, LANES), jnp.float32))
        started = reduce(phase, gather)
        while gather.phase < phases and gather.hop < n_row - 1:
            gather.advance()
        following.advance()
        for copy in started:
            copy.wait_send()
        gather.finish()


def shards(n_row, n_col, features, tile_values, tile_rows, tile_cols, tile_count, w_first, w_second):
    slots, tile = tile_values.shape[2], tile_values.shape[-1]
    node_dev, width = features.shape
    row_tiles = node_dev * n_col // tile
    chunks = width // LANES
    phases = 2 * chunks
    pairs_total = (slots + row_tiles) // 2
    n_q = n_col // 2
    steps = n_q.bit_length() - 1
    plan_width = -(-2 * pairs_total // LANES) * LANES
    half = node_dev // 2
    vmem = pl.BlockSpec(memory_space=pltpu.VMEM)
    smem = pl.BlockSpec(memory_space=pltpu.SMEM)
    bf16 = jnp.bfloat16
    dma = pltpu.SemaphoreType.DMA
    aggregate = pl.pallas_call(
        functools.partial(kernel, n_row, n_col, chunks, pairs_total),
        name="gcn",
        out_shape=jax.ShapeDtypeStruct((node_dev, width), bf16),
        in_specs=[smem] + [vmem] * 4 + [pl.BlockSpec(memory_space=pltpu.HBM)],
        out_specs=vmem,
        scratch_shapes=[pltpu.VMEM((n_row * node_dev // tile, tile, LANES), bf16)] * phases
        + [pltpu.VMEM((2 * n_q * half, LANES), bf16)] * phases
        + [pltpu.VMEM((2 * (n_q - 1) * half, LANES), bf16)] * phases
        + [
            pltpu.VMEM((slots + 1, tile, tile), bf16),
            pltpu.VMEM((pairs_total + 1, tile, LANES), bf16),
            pltpu.VMEM((n_col * node_dev, LANES), bf16),
            pltpu.VMEM((8, plan_width), jnp.int32),
            pltpu.VMEM((8, plan_width), jnp.float32),
            pltpu.SMEM((8, plan_width), jnp.int32),
            pltpu.SMEM((8, plan_width), jnp.float32),
            dma((2,)),
            dma((LOADS,)),
            dma((phases, 2, n_row - 1)),
            dma((phases, 2, n_row - 1)),
            dma((phases, 2, 2)),
            dma((phases, 2, 2)),
            dma((phases, 2, steps, 2)),
            dma((phases, 2, steps, 2)),
        ],
        compiler_params=pltpu.CompilerParams(
            collective_id=0, has_side_effects=True, vmem_limit_bytes=63 * 1024 * 1024
        ),
    )(tile_count, tile_rows[0], tile_cols[0], features, w_first, tile_values[0, 0])
    product = jnp.dot(aggregate, w_second, preferred_element_type=jnp.float32)
    return jax.nn.relu(product).astype(bf16)


def solution(mesh):
    return jax.shard_map(
        functools.partial(shards, mesh.shape["row"], mesh.shape["col"]),
        mesh=mesh,
        in_specs=(
            P(("row", "col"), None),
            P("row", "col", None, None, None),
            P("row", "col", None),
            P("row", "col", None),
            P("row", "col"),
            P(),
            P(),
        ),
        out_specs=P(("row", "col"), None),
        check_vma=False,
    )
```

```python
import functools

import jax
import jax.numpy as jnp
from jax import lax
from jax.experimental import pallas as pl
from jax.experimental.pallas import tpu as pltpu
from jax.sharding import PartitionSpec as P

LANES = 128
UNROLL = 8
LOADS = 4
PARTS = 2
ROWS_AT_ONCE = 256
MESH = pl.DeviceIdType.MESH


def iota(shape, axis):
    return lax.broadcasted_iota(jnp.int32, shape, axis)


def pair_plan(row_ids, col_ids, filled, row_tiles, pairs_total, width):
    slots = row_ids.shape[1]
    one, zero = jnp.int32(1), jnp.int32(0)

    def down(mask):
        return jnp.sum(mask, axis=0, keepdims=True)

    def across(mask):
        return jnp.sum(mask, axis=1, keepdims=True)

    square = (slots, slots)
    lane, sub = iota(square, 1), iota(square, 0)
    rows_l = jnp.where(iota((1, slots), 1) < filled, row_ids, -1)
    rows_s = across(jnp.where(lane == sub, rows_l, zero))
    cols_s = across(jnp.where(lane == sub, col_ids, zero))
    rank_s = across(jnp.where((rows_s == rows_l) & (lane < sub), one, zero))
    hit = jnp.where(rows_s == iota((slots, row_tiles), 1), one, zero)
    hit_t = jnp.where(rows_l == iota((row_tiles, slots), 0), one, zero)
    count_l, count_s = down(hit), across(hit_t)
    pairs_l, pairs_s = (count_l + 1) >> 1, (count_s + 1) >> 1
    box = (row_tiles, row_tiles)
    start_l = down(jnp.where(iota(box, 0) < iota(box, 1), pairs_s, zero))
    start_s = across(jnp.where(iota(box, 1) < iota(box, 0), pairs_l, zero))
    place_s = jnp.where(rows_s >= 0, 2 * across(hit * start_l) + rank_s, -one)
    here = place_s == iota((slots, width), 1)
    slot_ids = iota((slots, width), 0)
    slot_at = slots + down(jnp.where(here, slot_ids - slots, zero))
    col_at = down(jnp.where(here, cols_s, zero))
    opens = (start_s == iota((row_tiles, width), 1)) & (count_s > 0)
    keep = one - down(jnp.where(opens, one, zero))
    last = jnp.where(count_l > 0, start_l + pairs_l - 1, jnp.int32(pairs_total))
    return slot_at, col_at, keep.astype(jnp.float32), last


def kernel(n_row, n_col, chunks, pairs_total, filled, row_ids, col_ids, feat, w1, vals_hbm, out, *scratch):
    phases = 2 * chunks
    panels = scratch[:phases]
    core_in = scratch[phases : 2 * phases]
    step_in = scratch[2 * phases : 3 * phases]
    vals, sums, part, plan_v, keep_v, plan, keep, plan_sem = scratch[3 * phases : 3 * phases + 8]
    load_sem, g_send, g_recv, c_send, c_recv, s_send, s_recv = scratch[3 * phases + 8 :]
    slots, tile, _ = vals_hbm.shape
    node_dev, width = feat.shape
    per_dev = node_dev // tile
    half_tiles = per_dev // 2
    n_q = n_col // 2
    steps = n_q.bit_length() - 1
    block = half_tiles * tile
    half_rows = n_q * block
    r, c = lax.axis_index("row"), lax.axis_index("col")
    b0 = lax.rem(c, 2)
    q = lax.div(c, 2)

    barrier = pltpu.get_barrier_semaphore()
    partners = []
    for bit in range(steps + 1):
        mine = lax.rem(lax.div(c, 1 << bit), 2)
        partners.append((r, c + (1 - 2 * mine) * (1 << bit)))
    for device in partners:
        pl.semaphore_signal(barrier, inc=1, device_id=device, device_id_type=MESH)

    @pl.when(r > 0)
    def _():
        pl.semaphore_signal(barrier, inc=1, device_id=(r - 1, c), device_id_type=MESH)

    @pl.when(r < n_row - 1)
    def _():
        pl.semaphore_signal(barrier, inc=1, device_id=(r + 1, c), device_id_type=MESH)

    share = slots // LOADS
    loads = [
        pltpu.make_async_copy(
            vals_hbm.at[pl.ds(i * share, share)], vals.at[pl.ds(i * share, share)], load_sem.at[i]
        )
        for i in range(LOADS)
    ]
    for load in loads:
        load.start()

    def own(phase, offset, rows):
        return panels[phase].at[pl.ds(r * per_dev + offset, rows)]

    def project(chunk):
        def body(i, carry):
            at = pl.multiple_of(i * ROWS_AT_ONCE, ROWS_AT_ONCE)
            product = jnp.dot(
                feat[pl.ds(at, ROWS_AT_ONCE), :],
                w1[:, chunk * LANES : (chunk + 1) * LANES],
                preferred_element_type=jnp.float32,
            )
            tiles = ROWS_AT_ONCE // tile
            own(chunk, i * tiles, tiles)[...] = product.astype(jnp.bfloat16).reshape(
                tiles, tile, LANES
            )
            return carry

        lax.fori_loop(0, node_dev // ROWS_AT_ONCE, body, 0)

    project(0)
    neighbours = (r > 0).astype(jnp.int32) + (r < n_row - 1).astype(jnp.int32)
    pl.semaphore_wait(barrier, len(partners) + neighbours)

    cut = per_dev // PARTS

    def hop_copy(phase, way, hop, part_id, node, device):
        view = panels[phase].at[pl.ds(node * per_dev + part_id * cut, cut)]
        return pltpu.make_async_remote_copy(
            src_ref=view,
            dst_ref=view,
            send_sem=g_send.at[phase, way, hop - 1, part_id],
            recv_sem=g_recv.at[phase, way, hop - 1, part_id],
            device_id=(device, c),
            device_id_type=MESH,
        )

    def sends(phase, hop, k):
        yield (r < n_row - 1) & (r >= hop - 1), lambda: hop_copy(
            phase, 0, hop, k, r - hop + 1, r + 1
        )
        yield (r > 0) & (r + hop <= n_row), lambda: hop_copy(phase, 1, hop, k, r + hop - 1, r - 1)

    def hop_start(phase, hop, k):
        for cond, make in sends(phase, hop, k):

            @pl.when(cond)
            def _(make=make):
                make().start()

    def hop_wait(phase, hop, k):
        @pl.when(r >= hop)
        def _():
            hop_copy(phase, 0, hop, k, r - hop, r).wait_recv()

        @pl.when(r + hop < n_row)
        def _():
            hop_copy(phase, 1, hop, k, r + hop, r).wait_recv()

    def hop_drain(phase, hop, k):
        for cond, make in sends(phase, hop, k):

            @pl.when(cond)
            def _(make=make):
                make().wait_send()

    class Gather:
        def __init__(self, phase):
            self.phase, self.unit = phase, 0
            self.units = (n_row - 1) * PARTS if phase < phases else 0

        def advance(self, count=1):
            for _ in range(min(count, self.units - self.unit)):
                hop, k = self.unit // PARTS + 1, self.unit % PARTS
                if hop > 1:
                    hop_wait(self.phase, hop - 1, k)
                hop_start(self.phase, hop, k)
                self.unit += 1

        def send_all(self):
            self.advance(self.units)

        def finish(self):
            self.send_all()
            if self.units:
                for k in range(PARTS):
                    hop_wait(self.phase, n_row - 1, k)
                for hop in range(1, n_row):
                    for k in range(PARTS):
                        hop_drain(self.phase, hop, k)

    def compute(phase, low, high, total):
        panel = panels[phase]

        def one(p, acc):
            left = [vals[plan[0, 2 * p + k]] for k in range(2)]
            right = [panel[plan[1, 2 * p + k]] for k in range(2)]
            product = jnp.dot(
                jnp.concatenate(left, axis=1),
                jnp.concatenate(right, axis=0),
                preferred_element_type=jnp.float32,
            )
            acc = acc * keep[0, p] + product
            sums[p] = acc.astype(jnp.bfloat16)
            return acc

        def body(i, acc):
            for u in range(UNROLL):
                acc = one(i * UNROLL + u, acc)
            return acc

        return lax.fori_loop(low // UNROLL, high // UNROLL, body, total)

    def place_rows(parity):
        def body(i, carry):
            dq, h = lax.div(i, 2), lax.rem(i, 2)
            dest = 2 * dq + parity
            rev = sum(lax.rem(lax.div(dq, 1 << k), 2) * (1 << (steps - 1 - k)) for k in range(steps))
            at = rev * (1 - h) + dq * h
            base = ((parity * 2 + h) * n_q + at) * half_tiles
            for t in range(half_tiles):
                row_tile = dest * per_dev + h * half_tiles + t
                part[pl.ds(pl.multiple_of((base + t) * tile, tile), tile), :] = sums[
                    plan[2, row_tile]
                ]
            return carry

        lax.fori_loop(0, 2 * n_q, body, 0)

    def add_in(at, source, source_at, rows):
        piece = min(rows, ROWS_AT_ONCE)

        def body(i, carry):
            here = pl.ds(pl.multiple_of(at + i * piece, tile), piece)
            there = pl.ds(pl.multiple_of(source_at + i * piece, tile), piece)
            added = part[here, :].astype(jnp.float32) + source[there, :].astype(jnp.float32)
            part[here, :] = added.astype(jnp.bfloat16)
            return carry

        lax.fori_loop(0, rows // piece, body, 0)

    def remote(src, dst, send_sem, recv_sem, device):
        return pltpu.make_async_remote_copy(
            src_ref=src,
            dst_ref=dst,
            send_sem=send_sem,
            recv_sem=recv_sem,
            device_id=device,
            device_id_type=MESH,
        )

    def rows_at(ref, at, rows):
        return ref.at[pl.ds(pl.multiple_of(at, tile), rows)]

    def mine_at(h, step):
        return lax.rem(lax.div(q, 1 << (step if h == 0 else steps - 1 - step)), 2)

    def pieces(h, step, size):
        if step >= steps:
            return [(0, size)]
        mine = mine_at(h, step)
        return [((1 - mine) * (size // 2), size // 2), (mine * (size // 2), size // 2)]

    def reduce(phase, gather):
        place_rows(1 - b0)
        started = []
        cuts = [pieces(h, 0, half_rows) for h in range(2)]
        arrived = [[], []]
        for k in range(len(cuts[0])):
            for h in range(2):
                off, rows = cuts[h][k]
                copy = remote(
                    rows_at(part, ((1 - b0) * 2 + h) * half_rows + off, rows),
                    rows_at(core_in[phase], h * half_rows + off, rows),
                    c_send.at[phase, h, k],
                    c_recv.at[phase, h, k],
                    partners[0],
                )
                copy.start()
                started.append(copy)
                arrived[h].append((copy, core_in[phase], h * half_rows + off, off, rows))
        gather.advance()
        place_rows(b0)
        gather.advance()
        base = [(b0 * 2 + h) * half_rows for h in range(2)]

        def take(h, k):
            copy, source, source_at, off, rows = arrived[h][k]
            copy.wait_recv()
            add_in(base[h] + off, source, source_at, rows)

        size = half_rows
        for step in range(steps):
            following = [[], []]
            for h in range(2):
                take(h, 0)
                bit = step if h == 0 else steps - 1 - step
                away = base[h] + (1 - mine_at(h, step)) * (size // 2)
                landing = (h * (n_q - 1) + n_q - (n_q >> step)) * block
                for k, (off, rows) in enumerate(pieces(h, step + 1, size // 2)):
                    copy = remote(
                        rows_at(part, away + off, rows),
                        rows_at(step_in[phase], landing + off, rows),
                        s_send.at[phase, h, step, k],
                        s_recv.at[phase, h, step, k],
                        partners[1 + bit],
                    )
                    copy.start()
                    started.append(copy)
                    following[h].append((copy, step_in[phase], landing + off, off, rows))
            for h in range(2):
                take(h, 1)
                base[h] = base[h] + mine_at(h, step) * (size // 2)
            size //= 2
            arrived = following
            gather.advance()
        for h in range(2):
            copy, source, source_at, off, rows = arrived[h][0]
            copy.wait_recv()
            here = pl.ds(pl.multiple_of(base[h], tile), block)
            there = pl.ds(pl.multiple_of(source_at, tile), block)
            added = part[here, :].astype(jnp.float32) + source[there, :].astype(jnp.float32)
            if phase < chunks:
                hidden = jnp.maximum(added, 0.0).astype(jnp.bfloat16)
                own(phase + chunks, h * half_tiles, half_tiles)[...] = hidden.reshape(
                    half_tiles, tile, LANES
                )
            else:
                at = (phase - chunks) * LANES
                out[h * block : (h + 1) * block, at : at + LANES] = added.astype(jnp.bfloat16)
        return started

    vals[slots] = jnp.zeros((tile, tile), vals.dtype)
    sums[pairs_total] = jnp.zeros((tile, LANES), sums.dtype)
    gather = Gather(0)
    gather.advance(PARTS)
    for chunk in range(1, chunks):
        project(chunk)
    slot_at, col_at, keep_at, last = pair_plan(
        row_ids[...], col_ids[...], filled[0, 0], n_col * per_dev, pairs_total, plan.shape[1]
    )
    plan_v[0:1, :] = slot_at
    plan_v[1:2, :] = col_at
    plan_v[2:3, : last.shape[1]] = last
    keep_v[0:1, :] = keep_at
    moves = [
        pltpu.make_async_copy(plan_v, plan, plan_sem.at[0]),
        pltpu.make_async_copy(keep_v, keep, plan_sem.at[1]),
    ]
    gather.advance(PARTS)
    for move in moves:
        move.start()
    for move in moves:
        move.wait()
    for load in loads:
        load.wait()
    following = Gather(1)
    gather.send_all()
    following.advance(PARTS)
    gather.finish()
    for phase in range(phases):
        gather, following = following, Gather(phase + 2)
        middle = pairs_total // 2 // UNROLL * UNROLL
        total = compute(phase, 0, middle, jnp.zeros((tile, LANES), jnp.float32))
        gather.advance()
        compute(phase, middle, pairs_total, total)
        started = reduce(phase, gather)
        gather.send_all()
        following.advance(PARTS)
        for copy in started:
            copy.wait_send()
        gather.finish()


def shards(n_row, n_col, features, tile_values, tile_rows, tile_cols, tile_count, w_first, w_second):
    slots, tile = tile_values.shape[2], tile_values.shape[-1]
    node_dev, width = features.shape
    row_tiles = node_dev * n_col // tile
    chunks = width // LANES
    phases = 2 * chunks
    pairs_total = (slots + row_tiles) // 2
    n_q = n_col // 2
    steps = n_q.bit_length() - 1
    plan_width = -(-2 * pairs_total // LANES) * LANES
    half = node_dev // 2
    vmem = pl.BlockSpec(memory_space=pltpu.VMEM)
    smem = pl.BlockSpec(memory_space=pltpu.SMEM)
    bf16 = jnp.bfloat16
    dma = pltpu.SemaphoreType.DMA
    aggregate = pl.pallas_call(
        functools.partial(kernel, n_row, n_col, chunks, pairs_total),
        name="gcn",
        out_shape=jax.ShapeDtypeStruct((node_dev, width), bf16),
        in_specs=[smem] + [vmem] * 4 + [pl.BlockSpec(memory_space=pltpu.HBM)],
        out_specs=vmem,
        scratch_shapes=[pltpu.VMEM((n_row * node_dev // tile, tile, LANES), bf16)] * phases
        + [pltpu.VMEM((2 * n_q * half, LANES), bf16)] * phases
        + [pltpu.VMEM((2 * (n_q - 1) * half, LANES), bf16)] * phases
        + [
            pltpu.VMEM((slots + 1, tile, tile), bf16),
            pltpu.VMEM((pairs_total + 1, tile, LANES), bf16),
            pltpu.VMEM((n_col * node_dev, LANES), bf16),
            pltpu.VMEM((8, plan_width), jnp.int32),
            pltpu.VMEM((8, plan_width), jnp.float32),
            pltpu.SMEM((8, plan_width), jnp.int32),
            pltpu.SMEM((8, plan_width), jnp.float32),
            dma((2,)),
            dma((LOADS,)),
            dma((phases, 2, n_row - 1, PARTS)),
            dma((phases, 2, n_row - 1, PARTS)),
            dma((phases, 2, 2)),
            dma((phases, 2, 2)),
            dma((phases, 2, steps, 2)),
            dma((phases, 2, steps, 2)),
        ],
        compiler_params=pltpu.CompilerParams(
            collective_id=0, has_side_effects=True, vmem_limit_bytes=63 * 1024 * 1024
        ),
    )(tile_count, tile_rows[0], tile_cols[0], features, w_first, tile_values[0, 0])
    product = jnp.dot(aggregate, w_second, preferred_element_type=jnp.float32)
    return jax.nn.relu(product).astype(bf16)


def solution(mesh):
    return jax.shard_map(
        functools.partial(shards, mesh.shape["row"], mesh.shape["col"]),
        mesh=mesh,
        in_specs=(
            P(("row", "col"), None),
            P("row", "col", None, None, None),
            P("row", "col", None),
            P("row", "col", None),
            P("row", "col"),
            P(),
            P(),
        ),
        out_specs=P(("row", "col"), None),
        check_vma=False,
    )
```
